32 devices in a mesh: band: 8 (over z, x), ga: 4 (over y, core).
Axes of the slice: x: 2, y: 2, z: 4, core: 2. Of those that a mesh axis runs over, the one named last changes fastest.
Arguments:
- elements: bfloat16 [2, 768, 2048], P(None, 'band', 'ga'), may hold values from -0.75 to 0.75
- screened: bfloat16 [2, 2, 2048, 2048], P(None, None, 'ga'), may hold values from -0.09375 to 0.09375
- energies: float32 [768], replicated, may hold values from -3 to 3
- freq_points: float32 [2], replicated, may hold values from -3 to 3
- freq_weights: float32 [2], replicated, may hold values from 0.5 to 2
- band_of_slot: int32 [768], replicated, may hold values from 0 to 767, each once
Outputs:
- sigma: float32 [2, 768, 768], P(None, 'band', 'ga')
The draws below stay inside these ranges and needn't reach their ends.
Inputs may be any that keep to these rules, and one draw needn't show every extreme that they name: `band_of_slot`: each of 0 to 767 stands once.
All inputs are finite; a program needn't handle non-finite values.
Results may differ from the reference program's by a relative error of at most 0.0042.
Values may be sent and summed in bfloat16 or wider, within the bound.
A program may use at most 128 MiB of HBM per device.

```python
import math
import jax
import jax.numpy as jnp

NG = 2048
NW = 2
NB = 768


def block_levels(rng, extent, split, smallest, high):
    gain = 1.0
    for axis_at, blocks in split:
        heights = jax.random.uniform(jax.random.fold_in(jax.random.fold_in(rng, 6), axis_at), (blocks,), jnp.float32, smallest / len(split), high / len(split))
        gain = gain * jnp.repeat(jnp.exp(heights), extent[axis_at] // blocks).reshape((-1,) + (1,) * (len(extent) - 1 - axis_at))
    return gain


def normal_values(rng, dims, deviation, limit, shards=(), dtype=jnp.bfloat16):
    values = deviation * jax.random.normal(rng, dims, jnp.float32)
    if shards:
        values = values * block_levels(rng, dims, shards, -0.22, 0.18)
    return jnp.clip(values, -limit, limit).astype(dtype)


def setup_inputs(seed: int = 0) -> dict:
    keys = jax.random.split(jax.random.key(seed), 7)
    elements = normal_values(keys[0], (2, NB, NG), 0.125, 0.75, ((1, 8), (2, 4)))
    screened = normal_values(keys[1], (NW, 2, NG, NG), (2 * NG) ** -0.5, 0.09375, ((2, 4),))
    energies = jnp.clip(jax.random.uniform(keys[2], (NB,), jnp.float32, -3.0, 3.0), -3.0, 3.0)
    freq_points = jnp.clip(jax.random.uniform(keys[3], (NW,), jnp.float32, -3.0, 3.0), -3.0, 3.0)
    freq_weights = jnp.clip(jnp.exp(jax.random.uniform(keys[4], (NW,), jnp.float32, math.log(0.5), math.log(2.0))), 0.5, 2.0)
    band_of_slot = jax.random.permutation(keys[5], NB).astype(jnp.int32)
    return dict(elements=elements, screened=screened, energies=energies, freq_points=freq_points, freq_weights=freq_weights, band_of_slot=band_of_slot)


def reference(elements, screened, energies, freq_points, freq_weights, band_of_slot):
    slot_energy = jnp.take(energies, band_of_slot.astype(jnp.int32))
    offset = slot_energy[None, :] - freq_points[:, None]
    screen = freq_weights[:, None] / (1.0 + 4.0 * offset * offset)
    real_part = elements[0]
    imag_part = elements[1]
    total = jnp.zeros((2, NB, NB), jnp.float32)
    for freq in range(NW):
        w_real = screened[freq, 0]
        w_imag = screened[freq, 1]
        y_real = (jnp.dot(real_part, w_real.T, preferred_element_type=jnp.float32)
                  - jnp.dot(imag_part, w_imag.T, preferred_element_type=jnp.float32)).astype(jnp.bfloat16)
        y_imag = (jnp.dot(real_part, w_imag.T, preferred_element_type=jnp.float32)
                  + jnp.dot(imag_part, w_real.T, preferred_element_type=jnp.float32)).astype(jnp.bfloat16)
        pair_real = (jnp.dot(real_part, y_real.T, preferred_element_type=jnp.float32)
                     + jnp.dot(imag_part, y_imag.T, preferred_element_type=jnp.float32))
        pair_imag = (jnp.dot(real_part, y_imag.T, preferred_element_type=jnp.float32)
                     - jnp.dot(imag_part, y_real.T, preferred_element_type=jnp.float32))
        factor = 0.5 * (screen[freq][:, None] + screen[freq][None, :])
        total = total + factor[None] * jnp.stack([pair_real, pair_imag])
    return total
```

```python
import functools

import jax
import jax.numpy as jnp
from jax import lax
from jax.experimental import pallas as pl
from jax.experimental.pallas import tpu as pltpu
from jax.sharding import PartitionSpec as P

MESH = pl.DeviceIdType.MESH
F32 = jnp.float32
BF16 = jnp.bfloat16
NT = (((1,), (1,)), ((), ()))


def kernel(nb, ng, nx, el, wh, en, bos, fp, fw, out, *scratch):
    (gat, wv, a_ref, e3, scr, held, dsend, drecv, ysend, yrecv, lv, ssend, srecv, own,
     loc_sem, w_sem, up_sem, dn_sem, x_sem, g_recv, d_ss, d_rs, y_ss, y_rs, s_ss, s_rs) = scratch
    rows, depth = el.shape[1], el.shape[2]
    quarter = wh.shape[3] // ng
    nz, ny = nb // nx, ng // 2
    wide = nx * rows
    per = nz // ng
    slots = en.shape[1]
    b, g = lax.axis_index("band"), lax.axis_index("ga")
    z, x = b // nx, lax.rem(b, nx)
    y, c = g // 2, lax.rem(g, 2)
    mate = g + 1 - 2 * c
    xb = z * nx + (nx - 1 - x)

    mine = gat.at[:, pl.ds(pl.multiple_of(b * rows, rows), rows), :]
    local = pltpu.make_async_copy(el, mine, loc_sem)
    local.start()

    def q_of(other, d):
        core = (1 - c) if other else c
        return lax.rem(y + d, ny) * 2 + core

    order = []
    for d in list(range(1, ny)) + [0]:
        order += [(1, d), (0, d)]

    def w_copy(k, w):
        o, d = order[k]
        cols = pl.ds(pl.multiple_of(q_of(o, d) * quarter, quarter), quarter)
        return pltpu.make_async_copy(wh.at[w, :, :, cols], wv.at[w, k], w_sem.at[w, k])

    for k in range(ng):
        for w in range(2):
            w_copy(k, w).start()

    barrier = pltpu.get_barrier_semaphore()

    def greet(band, ga):
        pl.semaphore_signal(barrier, inc=1, device_id=(band, ga), device_id_type=MESH)

    for r in range(1, ng):
        greet(b, lax.rem(g + r, ng))
    greet(xb, g)

    @pl.when(z > 0)
    def _():
        greet(b - nx, g)

    @pl.when(z < nz - 1)
    def _():
        greet(b + nx, g)

    below = jnp.where(z > 0, 1, 0)
    above = jnp.where(z < nz - 1, 1, 0)
    pl.semaphore_wait(barrier, ng + below + above)
    local.wait()

    def block(src):
        return gat.at[:, pl.ds(pl.multiple_of(src * rows, rows), rows), :]

    def send(src, dst, sem):
        ref = block(src)
        return pltpu.make_async_remote_copy(
            src_ref=ref, dst_ref=ref, send_sem=sem, recv_sem=g_recv.at[src],
            device_id=(dst, g), device_id_type=MESH)

    def arrived(src):
        send(src, xb, x_sem.at[0]).wait_recv()

    def fwd_up(s):
        zs = z - s

        @pl.when(zs >= 0)
        def _():
            src = zs * nx + x
            if not (isinstance(s, int) and s == 0):
                arrived(src)

            @pl.when(z < nz - 1)
            def _():
                send(src, b + nx, up_sem.at[zs]).start()

            send(src, xb, x_sem.at[zs]).start()

    def fwd_down(s):
        zs = z + s

        @pl.when(zs < nz)
        def _():
            src = zs * nx + x
            if not (isinstance(s, int) and s == 0):
                arrived(src)

            @pl.when(z > 0)
            def _():
                send(src, b - nx, dn_sem.at[zs]).start()

            if not (isinstance(s, int) and s == 0):
                send(src, xb, x_sem.at[zs]).start()

    def fwd(s):
        fwd_up(s)
        fwd_down(s)

    fwd(0)

    er = gat[0, pl.ds(pl.multiple_of(b * rows, rows), rows), :]
    ei = gat[1, pl.ds(pl.multiple_of(b * rows, rows), rows), :]
    a_ref[:rows, :depth] = er
    a_ref[:rows, depth:] = ei
    a_ref[rows:, :depth] = -ei
    a_ref[rows:, depth:] = er

    def d_copy(d, w):
        return pltpu.make_async_remote_copy(
            src_ref=dsend.at[d, w], dst_ref=drecv.at[d, w], send_sem=d_ss.at[d, w],
            recv_sem=d_rs.at[d, w], device_id=(b, mate), device_id_type=MESH)

    def y_copy(d, w):
        return pltpu.make_async_remote_copy(
            src_ref=ysend.at[d - 1, w], dst_ref=yrecv.at[d - 1, w], send_sem=y_ss.at[d - 1, w],
            recv_sem=y_rs.at[d - 1, w], device_id=(b, lax.rem(y + d, ny) * 2 + c),
            device_id_type=MESH)

    def pass_on(d):
        for w in range(2):
            d_copy(d, w).wait_recv()
            ysend[d - 1, w] = (held[d, w] + drecv[d, w].astype(F32)).astype(BF16)
            y_copy(d, w).start()

    for k in range(ng):
        o, d = order[k]
        for w in range(2):
            w_copy(k, w).wait()
            part = jnp.dot(a_ref[...], wv[w, k].reshape(2 * depth, quarter),
                           preferred_element_type=F32)
            if o:
                dsend[d, w] = part.astype(BF16)
                d_copy(d, w).start()
            else:
                held[d, w] = part
        if o and k >= 2:
            pass_on(order[k - 1][1])

    row = lax.broadcasted_iota(jnp.int32, (16, slots), 0)
    e = en[...]
    hi = e.astype(BF16).astype(F32)
    mid = (e - hi).astype(BF16).astype(F32)
    lo = e - hi - mid
    e3[...] = jnp.where(row == 0, hi, jnp.where(row == 1, mid, jnp.where(row == 2, lo, 0.0))).astype(BF16)
    tile = slots if slots <= 1024 else 8 * rows

    def plane_screen(i, carry):
        slot = bos[i]

        def add(j, acc):
            at = pl.multiple_of(j * tile, tile)
            hit = lax.broadcasted_iota(jnp.int32, (tile, wide), 0) + at == slot
            return acc + jnp.dot(e3[:, pl.ds(at, tile)], jnp.where(hit, 1.0, 0.0).astype(BF16),
                                 preferred_element_type=F32)

        acc = lax.fori_loop(0, slots // tile, add, jnp.zeros((16, wide), F32))
        energy = jnp.sum(acc, axis=0, keepdims=True)
        for w in range(2):
            off = energy - fp[w]
            scr[i, w : w + 1, :] = 0.5 * (fw[w] / (1.0 + 4.0 * off * off))
        return carry

    lax.fori_loop(0, nz, plane_screen, 0)
    pick = lax.broadcasted_iota(jnp.int32, (rows, wide), 1) == (
        lax.broadcasted_iota(jnp.int32, (rows, wide), 0) + x * rows)
    cols = [jnp.sum(jnp.where(pick, scr[z, w : w + 1, :], 0.0), axis=1, keepdims=True)
            for w in range(2)]

    def consume_plane(zs):
        at = pl.ds(pl.multiple_of(zs * wide, wide), wide)
        pr = lax.dot_general(lv[0], gat[0, at, :], NT, preferred_element_type=F32)
        pr = pr + lax.dot_general(lv[1], gat[1, at, :], NT, preferred_element_type=F32)
        f = [cols[w] + scr[zs, w : w + 1, :] for w in range(2)]
        total = [f[0] * pr[i * rows : (i + 1) * rows]
                 + f[1] * pr[(2 + i) * rows : (3 + i) * rows] for i in range(2)]
        q, p = zs // per, lax.rem(zs, per)

        @pl.when(q == g)
        def _():
            for i in range(2):
                own[p, i] = total[i]

        @pl.when(q != g)
        def _():
            for i in range(2):
                ssend[zs, i] = total[i]
            slot = lax.rem(g - q + ng, ng) - 1
            pltpu.make_async_remote_copy(
                src_ref=ssend.at[zs], dst_ref=srecv.at[slot, p], send_sem=s_ss.at[zs],
                recv_sem=s_rs.at[slot, p], device_id=(b, q), device_id_type=MESH).start()

    def consume(s):
        @pl.when(z - s >= 0)
        def _():
            arrived((z - s) * nx + (nx - 1 - x))
            consume_plane(z - s)

        if not (isinstance(s, int) and s == 0):
            @pl.when(z + s < nz)
            def _():
                arrived((z + s) * nx + (nx - 1 - x))
                consume_plane(z + s)

    fwd(1)
    if nz > 2:
        fwd(2)

    for w in range(2):
        total = held[0, w]
        d_copy(0, w).wait_recv()
        total = total + drecv[0, w].astype(F32)
        for d in range(1, ny):
            y_copy(d, w).wait_recv()
            total = total + yrecv[d - 1, w].astype(F32)
        total = total.astype(BF16)
        lv[0, 2 * w * rows : 2 * (w + 1) * rows, :] = total
        lv[1, 2 * w * rows : (2 * w + 1) * rows, :] = -total[rows:]
        lv[1, (2 * w + 1) * rows : (2 * w + 2) * rows, :] = total[:rows]

    consume(0)

    def tail(s, carry):
        consume(s - 2)
        fwd(s)
        return carry

    lax.fori_loop(3, nz, tail, 0)
    for s in range(max(1, nz - 2), nz):
        consume(s)

    def sent(zs, carry):
        src = zs * nx + x

        @pl.when((zs <= z) & (z < nz - 1))
        def _():
            send(src, b + nx, up_sem.at[zs]).wait_send()

        @pl.when((zs >= z) & (z > 0))
        def _():
            send(src, b - nx, dn_sem.at[zs]).wait_send()

        send(src, xb, x_sem.at[zs]).wait_send()

        @pl.when(zs // per != g)
        def _():
            pltpu.make_async_remote_copy(
                src_ref=ssend.at[zs], dst_ref=srecv.at[0, 0], send_sem=s_ss.at[zs],
                recv_sem=s_rs.at[0, 0], device_id=(b, mate), device_id_type=MESH).wait_send()

        return carry

    lax.fori_loop(0, nz, sent, 0)
    for w in range(2):
        for d in range(ny):
            d_copy(d, w).wait_send()
        for d in range(1, ny):
            y_copy(d, w).wait_send()

    def finish(p, carry):
        total = own[p]
        for r in range(ng - 1):
            pltpu.make_async_remote_copy(
                src_ref=ssend.at[0], dst_ref=srecv.at[r, p], send_sem=s_ss.at[0],
                recv_sem=s_rs.at[r, p], device_id=(b, mate), device_id_type=MESH).wait_recv()
            total = total + srecv[r, p]
        out[p] = total
        return carry

    lax.fori_loop(0, per, finish, 0)


def solution(mesh):
    nb, ng = mesh.shape["band"], mesh.shape["ga"]
    nx = 2
    nz = nb // nx
    ny = ng // 2
    per = nz // ng

    def step(elements, screened, energies, freq_points, freq_weights, band_of_slot):
        _, rows, depth = elements.shape
        quarter = screened.shape[3] // ng
        slots = energies.shape[0]
        wide = nx * rows
        any_space = pl.BlockSpec(memory_space=pl.ANY)
        vmem = pl.BlockSpec(memory_space=pltpu.VMEM)
        smem = pl.BlockSpec(memory_space=pltpu.SMEM)
        dma = pltpu.SemaphoreType.DMA
        result = pl.pallas_call(
            functools.partial(kernel, nb, ng, nx),
            out_shape=jax.ShapeDtypeStruct((per, 2, rows, wide), F32),
            in_specs=[any_space, any_space, vmem, vmem, smem, smem],
            out_specs=vmem,
            scratch_shapes=[
                pltpu.VMEM((2, nb * rows, depth), BF16),
                pltpu.VMEM((2, ng, 2, depth, quarter), BF16),
                pltpu.VMEM((2 * rows, 2 * depth), BF16),
                pltpu.VMEM((16, slots), BF16),
                pltpu.VMEM((nz, 2, wide), F32),
                pltpu.VMEM((ny, 2, 2 * rows, quarter), F32),
                pltpu.VMEM((ny, 2, 2 * rows, quarter), BF16),
                pltpu.VMEM((ny, 2, 2 * rows, quarter), BF16),
                pltpu.VMEM((ny - 1, 2, 2 * rows, quarter), BF16),
                pltpu.VMEM((ny - 1, 2, 2 * rows, quarter), BF16),
                pltpu.VMEM((2, 4 * rows, quarter), BF16),
                pltpu.VMEM((nz, 2, rows, wide), F32),
                pltpu.VMEM((ng - 1, per, 2, rows, wide), F32),
                pltpu.VMEM((per, 2, rows, wide), F32),
                dma, dma((2, ng)), dma((nz,)), dma((nz,)), dma((nz,)), dma((nb,)),
                dma((ny, 2)), dma((ny, 2)), dma((ny - 1, 2)), dma((ny - 1, 2)),
                dma((nz,)), dma((ng - 1, per)),
            ],
            compiler_params=pltpu.CompilerParams(
                collective_id=0, has_side_effects=True, vmem_limit_bytes=60 * 1024 * 1024),
        )(elements, screened, energies.reshape(1, slots), band_of_slot.reshape(nz, 1, wide),
          freq_points, freq_weights)
        return jnp.transpose(result, (1, 2, 0, 3)).reshape(2, rows, per * wide)

    placed = (P(None, "band", "ga"), P(None, None, "ga", None), P(), P(), P(), P())
    return jax.shard_map(
        step, mesh=mesh, in_specs=placed, out_specs=P(None, "band", "ga"), check_vma=False
    )
```

```python
import functools

import jax
import jax.numpy as jnp
from jax import lax
from jax.experimental import pallas as pl
from jax.experimental.pallas import tpu as pltpu
from jax.sharding import PartitionSpec as P

MESH = pl.DeviceIdType.MESH
F32 = jnp.float32
BF16 = jnp.bfloat16
NT = (((1,), (1,)), ((), ()))


def kernel(nb, ng, nx, el, wh, en, bos, fp, fw, out, *scratch):
    (gat, wv, a_ref, e3, scr, held, dsend, drecv, ysend, yrecv, lv, ssend, srecv, own,
     loc_sem, w_sem, up_sem, dn_sem, x_sem, g_recv, d_ss, d_rs, y_ss, y_rs, s_ss, s_rs) = scratch
    rows, depth = el.shape[1], el.shape[2]
    quarter = wh.shape[3] // ng
    nz, ny = nb // nx, ng // 2
    per = nb // ng
    slots = en.shape[0]
    b, g = lax.axis_index("band"), lax.axis_index("ga")
    z, x = b // nx, lax.rem(b, nx)
    y, c = g // 2, lax.rem(g, 2)
    mate = g + 1 - 2 * c
    xb = z * nx + (nx - 1 - x)

    barrier = pltpu.get_barrier_semaphore()

    def greet(band, ga):
        pl.semaphore_signal(barrier, inc=1, device_id=(band, ga), device_id_type=MESH)

    greet(xb, g)

    @pl.when(z > 0)
    def _():
        greet(b - nx, g)

    @pl.when(z < nz - 1)
    def _():
        greet(b + nx, g)

    for r in range(1, ng):
        greet(b, lax.rem(g + r, ng))

    mine = gat.at[:, pl.ds(pl.multiple_of(b * rows, rows), rows), :]
    local = pltpu.make_async_copy(el, mine, loc_sem)
    local.start()

    def q_of(other, d):
        core = (1 - c) if other else c
        return lax.rem(y + d, ny) * 2 + core

    order = []
    for d in list(range(1, ny)) + [0]:
        order += [(1, d), (0, d)]

    def w_copy(k, w):
        o, d = order[k]
        cols = pl.ds(pl.multiple_of(q_of(o, d) * quarter, quarter), quarter)
        return pltpu.make_async_copy(wh.at[w, :, :, cols], wv.at[w, k], w_sem.at[w, k])

    below = jnp.where(z > 0, 1, 0)
    above = jnp.where(z < nz - 1, 1, 0)
    pl.semaphore_wait(barrier, ng + below + above)
    local.wait()

    def send(src, i, dst, sem):
        ref = gat.at[i, pl.ds(pl.multiple_of(src * rows, rows), rows), :]
        return pltpu.make_async_remote_copy(
            src_ref=ref, dst_ref=ref, send_sem=sem, recv_sem=g_recv.at[src, i],
            device_id=(dst, g), device_id_type=MESH)

    def arrived(src, i):
        send(src, i, xb, x_sem.at[0, i]).wait_recv()

    def fwd_one(s, i, zs, ok, up, down):
        @pl.when(ok)
        def _():
            src = zs * nx + x
            if not (isinstance(s, int) and s == 0):
                arrived(src, i)
            if up:
                @pl.when(z < nz - 1)
                def _():
                    send(src, i, b + nx, up_sem.at[zs, i]).start()

            if down:
                @pl.when(z > 0)
                def _():
                    send(src, i, b - nx, dn_sem.at[zs, i]).start()

            send(src, i, xb, x_sem.at[zs, i]).start()

    def fwd(s):
        for i in range(2):
            if isinstance(s, int) and s == 0:
                fwd_one(0, i, z, z >= 0, True, True)
            else:
                fwd_one(s, i, z - s, z - s >= 0, True, False)
                fwd_one(s, i, z + s, z + s < nz, False, True)

    fwd(0)
    for k in range(ng):
        for w in range(2):
            w_copy(k, w).start()

    row = lax.broadcasted_iota(jnp.int32, (16, slots), 0)
    e = en[...].reshape(1, slots)
    hi = e.astype(BF16).astype(F32)
    mid = (e - hi).astype(BF16).astype(F32)
    lo = e - hi - mid
    e3[...] = jnp.where(row == 0, hi, jnp.where(row == 1, mid, jnp.where(row == 2, lo, 0.0))).astype(BF16)
    tile = slots if slots <= 1024 else 8 * rows

    for u in range(slots // tile):
        slot = bos[u * tile : (u + 1) * tile].reshape(1, tile)

        def add(j, acc):
            at = pl.multiple_of(j * tile, tile)
            hit = lax.broadcasted_iota(jnp.int32, (tile, tile), 0) + at == slot
            return acc + jnp.dot(e3[:, pl.ds(at, tile)], jnp.where(hit, 1.0, 0.0).astype(BF16),
                                 preferred_element_type=F32)

        acc = lax.fori_loop(0, slots // tile, add, jnp.zeros((16, tile), F32))
        energy = jnp.sum(acc, axis=0, keepdims=True)
        for w in range(2):
            off = energy - fp[w]
            value = 0.5 * (fw[w] / (1.0 + 4.0 * off * off))
            for v in range(tile // rows):
                scr[u * (tile // rows) + v, w : w + 1, :] = value[:, v * rows : (v + 1) * rows]
    pick = lax.broadcasted_iota(jnp.int32, (rows, rows), 1) == lax.broadcasted_iota(
        jnp.int32, (rows, rows), 0)
    cols = [jnp.sum(jnp.where(pick, scr[b, w : w + 1, :], 0.0), axis=1, keepdims=True)
            for w in range(2)]

    er = gat[0, pl.ds(pl.multiple_of(b * rows, rows), rows), :]
    ei = gat[1, pl.ds(pl.multiple_of(b * rows, rows), rows), :]
    a_ref[:rows, :depth] = er
    a_ref[:rows, depth:] = ei
    a_ref[rows:, :depth] = -ei
    a_ref[rows:, depth:] = er

    def d_copy(d, w):
        return pltpu.make_async_remote_copy(
            src_ref=dsend.at[d, w], dst_ref=drecv.at[d, w], send_sem=d_ss.at[d, w],
            recv_sem=d_rs.at[d, w], device_id=(b, mate), device_id_type=MESH)

    def y_copy(d, w):
        return pltpu.make_async_remote_copy(
            src_ref=ysend.at[d - 1, w], dst_ref=yrecv.at[d - 1, w], send_sem=y_ss.at[d - 1, w],
            recv_sem=y_rs.at[d - 1, w], device_id=(b, lax.rem(y + d, ny) * 2 + c),
            device_id_type=MESH)

    def pass_on(d):
        for w in range(2):
            d_copy(d, w).wait_recv()
            ysend[d - 1, w] = (held[d, w] + drecv[d, w].astype(F32)).astype(BF16)
            y_copy(d, w).start()

    for k in range(ng):
        o, d = order[k]
        for w in range(2):
            w_copy(k, w).wait()
            part = jnp.dot(a_ref[...], wv[w, k].reshape(2 * depth, quarter),
                           preferred_element_type=F32)
            if o:
                dsend[d, w] = part.astype(BF16)
                d_copy(d, w).start()
            else:
                held[d, w] = part
        if o and k >= 2:
            pass_on(order[k - 1][1])

    def consume_block(k):
        at = pl.ds(pl.multiple_of(k * rows, rows), rows)
        pr = lax.dot_general(lv[0], gat[0, at, :], NT, preferred_element_type=F32)
        pr = pr + lax.dot_general(lv[1], gat[1, at, :], NT, preferred_element_type=F32)
        f = [cols[w] + scr[k, w : w + 1, :] for w in range(2)]
        total = [f[0] * pr[i * rows : (i + 1) * rows]
                 + f[1] * pr[(2 + i) * rows : (3 + i) * rows] for i in range(2)]
        q, p = k // per, lax.rem(k, per)

        @pl.when(q == g)
        def _():
            for i in range(2):
                own[p, i] = total[i]

        @pl.when(q != g)
        def _():
            for i in range(2):
                ssend[k, i] = total[i].astype(BF16)
            slot = lax.rem(g - q + ng, ng) - 1
            pltpu.make_async_remote_copy(
                src_ref=ssend.at[k], dst_ref=srecv.at[slot, p], send_sem=s_ss.at[k],
                recv_sem=s_rs.at[slot, p], device_id=(b, q), device_id_type=MESH).start()

    def each_side(s, act):
        @pl.when(z - s >= 0)
        def _():
            act(z - s)

        if not (isinstance(s, int) and s == 0):
            @pl.when(z + s < nz)
            def _():
                act(z + s)

    def consume_own(s):
        each_side(s, lambda zs: consume_block(zs * nx + x))

    def consume_other(s):
        def act(zs):
            k = zs * nx + (nx - 1 - x)
            for i in range(2):
                arrived(k, i)
            consume_block(k)

        each_side(s, act)

    ahead = min(3, nz - 1)
    for s in range(1, ahead + 1):
        fwd(s)

    for w in range(2):
        total = held[0, w]
        d_copy(0, w).wait_recv()
        total = total + drecv[0, w].astype(F32)
        for d in range(1, ny):
            y_copy(d, w).wait_recv()
            total = total + yrecv[d - 1, w].astype(F32)
        total = total.astype(BF16)
        lv[0, 2 * w * rows : 2 * (w + 1) * rows, :] = total
        lv[1, 2 * w * rows : (2 * w + 1) * rows, :] = -total[rows:]
        lv[1, (2 * w + 1) * rows : (2 * w + 2) * rows, :] = total[:rows]

    for s in range(ahead + 1):
        consume_own(s)

    consume_other(0)

    def tail(s, carry):
        fwd(s)
        consume_own(s)
        consume_other(s - ahead)
        return carry

    lax.fori_loop(ahead + 1, nz, tail, 0)
    for s in range(nz - ahead, nz):
        consume_other(s)

    def sent(zs, carry):
        src = zs * nx + x
        for i in range(2):
            @pl.when((zs <= z) & (z < nz - 1))
            def _():
                send(src, i, b + nx, up_sem.at[zs, i]).wait_send()

            @pl.when((zs >= z) & (z > 0))
            def _():
                send(src, i, b - nx, dn_sem.at[zs, i]).wait_send()

            send(src, i, xb, x_sem.at[zs, i]).wait_send()
        for v in range(nx):
            k = zs * nx + v

            @pl.when(k // per != g)
            def _():
                pltpu.make_async_remote_copy(
                    src_ref=ssend.at[k], dst_ref=srecv.at[0, 0], send_sem=s_ss.at[k],
                    recv_sem=s_rs.at[0, 0], device_id=(b, mate), device_id_type=MESH).wait_send()

        return carry

    lax.fori_loop(0, nz, sent, 0)
    for w in range(2):
        for d in range(ny):
            d_copy(d, w).wait_send()
        for d in range(1, ny):
            y_copy(d, w).wait_send()

    for p in range(per):
        for r in range(ng - 1):
            pltpu.make_async_remote_copy(
                src_ref=ssend.at[0], dst_ref=srecv.at[r, p], send_sem=s_ss.at[0],
                recv_sem=s_rs.at[r, p], device_id=(b, mate), device_id_type=MESH).wait_recv()
        for i in range(2):
            total = own[p, i]
            for r in range(ng - 1):
                total = total + srecv[r, p, i].astype(F32)
            out[i, :, p * rows : (p + 1) * rows] = total


def solution(mesh):
    nb, ng = mesh.shape["band"], mesh.shape["ga"]
    nx = 2
    nz = nb // nx
    ny = ng // 2
    per = nb // ng

    def step(elements, screened, energies, freq_points, freq_weights, band_of_slot):
        _, rows, depth = elements.shape
        quarter = screened.shape[3] // ng
        slots = energies.shape[0]
        any_space = pl.BlockSpec(memory_space=pl.ANY)
        vmem = pl.BlockSpec(memory_space=pltpu.VMEM)
        smem = pl.BlockSpec(memory_space=pltpu.SMEM)
        dma = pltpu.SemaphoreType.DMA
        result = pl.pallas_call(
            functools.partial(kernel, nb, ng, nx),
            out_shape=jax.ShapeDtypeStruct((2, rows, per * rows), F32),
            in_specs=[any_space, any_space, vmem, vmem, smem, smem],
            out_specs=vmem,
            scratch_shapes=[
                pltpu.VMEM((2, nb * rows, depth), BF16),
                pltpu.VMEM((2, ng, 2, depth, quarter), BF16),
                pltpu.VMEM((2 * rows, 2 * depth), BF16),
                pltpu.VMEM((16, slots), BF16),
                pltpu.VMEM((nb, 2, rows), F32),
                pltpu.VMEM((ny, 2, 2 * rows, quarter), F32),
                pltpu.VMEM((ny, 2, 2 * rows, quarter), BF16),
                pltpu.VMEM((ny, 2, 2 * rows, quarter), BF16),
                pltpu.VMEM((ny - 1, 2, 2 * rows, quarter), BF16),
                pltpu.VMEM((ny - 1, 2, 2 * rows, quarter), BF16),
                pltpu.VMEM((2, 4 * rows, quarter), BF16),
                pltpu.VMEM((nb, 2, rows, rows), BF16),
                pltpu.VMEM((ng - 1, per, 2, rows, rows), BF16),
                pltpu.VMEM((per, 2, rows, rows), F32),
                dma, dma((2, ng)), dma((nz, 2)), dma((nz, 2)), dma((nz, 2)), dma((nb, 2)),
                dma((ny, 2)), dma((ny, 2)), dma((ny - 1, 2)), dma((ny - 1, 2)),
                dma((nb,)), dma((ng - 1, per)),
            ],
            compiler_params=pltpu.CompilerParams(
                collective_id=0, has_side_effects=True, vmem_limit_bytes=60 * 1024 * 1024),
        )(elements, screened, energies, band_of_slot, freq_points, freq_weights)
        return result

    placed = (P(None, "band", "ga"), P(None, None, "ga", None), P(), P(), P(), P())
    return jax.shard_map(
        step, mesh=mesh, in_specs=placed, out_specs=P(None, "band", "ga"), check_vma=False
    )
```

```python
import functools

import jax
import jax.numpy as jnp
from jax import lax
from jax.experimental import pallas as pl
from jax.experimental.pallas import tpu as pltpu
from jax.sharding import PartitionSpec as P

MESH = pl.DeviceIdType.MESH
F32 = jnp.float32
BF16 = jnp.bfloat16
NT = (((1,), (1,)), ((), ()))


def kernel(nb, ng, nx, el, wh, en_h, bos_h, fp_h, fw_h, out, *scratch):
    (en, bos, fp, fw, in_sem, gat, wv, a_ref, e3, scr, held, dsend, drecv, ysend, yrecv, lv, ssend, srecv, own,
     loc_sem, w_sem, up_sem, dn_sem, x_sem, g_recv, d_ss, d_rs, y_ss, y_rs, s_ss, s_rs) = scratch
    rows, depth = el.shape[1], el.shape[2]
    quarter = wh.shape[3] // ng
    nz, ny = nb // nx, ng // 2
    per = nb // ng
    slots = en.shape[0]
    b, g = lax.axis_index("band"), lax.axis_index("ga")
    z, x = b // nx, lax.rem(b, nx)
    y, c = g // 2, lax.rem(g, 2)
    mate = g + 1 - 2 * c
    xb = z * nx + (nx - 1 - x)

    barrier = pltpu.get_barrier_semaphore()

    def greet(band, ga):
        pl.semaphore_signal(barrier, inc=1, device_id=(band, ga), device_id_type=MESH)

    greet(xb, g)

    @pl.when(z > 0)
    def _():
        greet(b - nx, g)

    @pl.when(z < nz - 1)
    def _():
        greet(b + nx, g)

    for r in range(1, ng):
        greet(b, lax.rem(g + r, ng))

    small = [pltpu.make_async_copy(s, t, in_sem.at[i]) for i, (s, t) in enumerate(
        ((en_h, en), (bos_h, bos), (fp_h, fp), (fw_h, fw)))]
    mine = gat.at[:, pl.ds(pl.multiple_of(b * rows, rows), rows), :]
    local = pltpu.make_async_copy(el, mine, loc_sem)
    local.start()
    for copy in small:
        copy.start()

    def q_of(other, d):
        core = (1 - c) if other else c
        return lax.rem(y + d, ny) * 2 + core

    order = []
    for d in list(range(1, ny)) + [0]:
        order += [(1, d), (0, d)]

    def w_copy(k, w):
        o, d = order[k]
        cols = pl.ds(pl.multiple_of(q_of(o, d) * quarter, quarter), quarter)
        return pltpu.make_async_copy(wh.at[w, :, :, cols], wv.at[w, k], w_sem.at[w, k])

    below = jnp.where(z > 0, 1, 0)
    above = jnp.where(z < nz - 1, 1, 0)
    pl.semaphore_wait(barrier, ng + below + above)
    local.wait()

    unit = rows // 6
    pieces = ((0, 2 * unit), (2 * unit, 2 * unit), (4 * unit, unit), (5 * unit, unit))
    last = len(pieces) - 1

    def send(src, i, dst, sem):
        start, size = pieces[i]
        ref = gat.at[:, pl.ds(pl.multiple_of(src * rows + start, unit), size), :]
        return pltpu.make_async_remote_copy(
            src_ref=ref, dst_ref=ref, send_sem=sem, recv_sem=g_recv.at[src, i],
            device_id=(dst, g), device_id_type=MESH)

    def arrived(src, i):
        send(src, i, xb, x_sem.at[0, i]).wait_recv()

    def send_z(src, i, up, down):
        if up:
            @pl.when(z < nz - 1)
            def _():
                send(src, i, b + nx, up_sem.at[src, i]).start()

        if down:
            @pl.when(z > 0)
            def _():
                send(src, i, b - nx, dn_sem.at[src, i]).start()

    def fwd(s):
        for i in range(last):
            for zs, up in ((z - s, True), (z + s, False)):
                @pl.when((zs >= 0) & (zs < nz))
                def _():
                    src = zs * nx + x
                    arrived(src, i)
                    send_z(src, i, up, not up)
                    send(src, i, xb, x_sem.at[zs, i]).start()

    def fwd_last(s):
        for zs, up in ((z - s, True), (z + s, False)):
            @pl.when((zs >= 0) & (zs < nz))
            def _():
                for v in (x, nx - 1 - x):
                    arrived(zs * nx + v, last)
                    send_z(zs * nx + v, last, up, not up)

    send(b, last, xb, x_sem.at[z, last]).start()
    for i in range(last + 1):
        send_z(b, i, True, True)
        if i < last:
            send(b, i, xb, x_sem.at[z, i]).start()
    for k in range(ng):
        for w in range(2):
            w_copy(k, w).start()

    for copy in small:
        copy.wait()
    row = lax.broadcasted_iota(jnp.int32, (16, slots), 0)
    e = en[...].reshape(1, slots)
    hi = e.astype(BF16).astype(F32)
    mid = (e - hi).astype(BF16).astype(F32)
    lo = e - hi - mid
    e3[...] = jnp.where(row == 0, hi, jnp.where(row == 1, mid, jnp.where(row == 2, lo, 0.0))).astype(BF16)
    tile = slots if slots <= 1024 else 8 * rows

    for u in range(slots // tile):
        slot = bos[u * tile : (u + 1) * tile].reshape(1, tile)

        def add(j, acc):
            at = pl.multiple_of(j * tile, tile)
            hit = lax.broadcasted_iota(jnp.int32, (tile, tile), 0) + at == slot
            return acc + jnp.dot(e3[:, pl.ds(at, tile)], jnp.where(hit, 1.0, 0.0).astype(BF16),
                                 preferred_element_type=F32)

        acc = lax.fori_loop(0, slots // tile, add, jnp.zeros((16, tile), F32))
        energy = jnp.sum(acc, axis=0, keepdims=True)
        for w in range(2):
            off = energy - fp[w]
            value = 0.5 * (fw[w] / (1.0 + 4.0 * off * off))
            for v in range(tile // rows):
                scr[u * (tile // rows) + v, w : w + 1, :] = value[:, v * rows : (v + 1) * rows]
    pick = lax.broadcasted_iota(jnp.int32, (rows, rows), 1) == lax.broadcasted_iota(
        jnp.int32, (rows, rows), 0)
    cols = [jnp.sum(jnp.where(pick, scr[b, w : w + 1, :], 0.0), axis=1, keepdims=True)
            for w in range(2)]

    er = gat[0, pl.ds(pl.multiple_of(b * rows, rows), rows), :]
    ei = gat[1, pl.ds(pl.multiple_of(b * rows, rows), rows), :]
    a_ref[:rows, :depth] = er
    a_ref[:rows, depth:] = ei
    a_ref[rows:, :depth] = -ei
    a_ref[rows:, depth:] = er

    def d_copy(d, w):
        return pltpu.make_async_remote_copy(
            src_ref=dsend.at[d, w], dst_ref=drecv.at[d, w], send_sem=d_ss.at[d, w],
            recv_sem=d_rs.at[d, w], device_id=(b, mate), device_id_type=MESH)

    def y_copy(d, w):
        return pltpu.make_async_remote_copy(
            src_ref=ysend.at[d - 1, w], dst_ref=yrecv.at[d - 1, w], send_sem=y_ss.at[d - 1, w],
            recv_sem=y_rs.at[d - 1, w], device_id=(b, lax.rem(y + d, ny) * 2 + c),
            device_id_type=MESH)

    def pass_on(d):
        for w in range(2):
            d_copy(d, w).wait_recv()
            ysend[d - 1, w] = (held[d, w] + drecv[d, w].astype(F32)).astype(BF16)
            y_copy(d, w).start()

    for k in range(ng):
        o, d = order[k]
        for w in range(2):
            w_copy(k, w).wait()
            part = jnp.dot(a_ref[...], wv[w, k].reshape(2 * depth, quarter),
                           preferred_element_type=F32)
            if o:
                dsend[d, w] = part.astype(BF16)
                d_copy(d, w).start()
            else:
                held[d, w] = part
        if o and k >= 2:
            pass_on(order[k - 1][1])

    def consume_block(k):
        at = pl.ds(pl.multiple_of(k * rows, rows), rows)
        pr = lax.dot_general(lv[0], gat[0, at, :], NT, preferred_element_type=F32)
        pr = pr + lax.dot_general(lv[1], gat[1, at, :], NT, preferred_element_type=F32)
        f = [cols[w] + scr[k, w : w + 1, :] for w in range(2)]
        total = [f[0] * pr[i * rows : (i + 1) * rows]
                 + f[1] * pr[(2 + i) * rows : (3 + i) * rows] for i in range(2)]
        q, p = k // per, lax.rem(k, per)

        @pl.when(q == g)
        def _():
            for i in range(2):
                own[p, i] = total[i]

        @pl.when(q != g)
        def _():
            for i in range(2):
                ssend[k, i] = total[i].astype(BF16)
            slot = lax.rem(g - q + ng, ng) - 1
            pltpu.make_async_remote_copy(
                src_ref=ssend.at[k], dst_ref=srecv.at[slot, p], send_sem=s_ss.at[k],
                recv_sem=s_rs.at[slot, p], device_id=(b, q), device_id_type=MESH).start()

    def each_side(s, act):
        @pl.when(z - s >= 0)
        def _():
            act(z - s)

        if not (isinstance(s, int) and s == 0):
            @pl.when(z + s < nz)
            def _():
                act(z + s)

    def consume_own(s):
        each_side(s, lambda zs: consume_block(zs * nx + x))

    def consume_other(s):
        def act(zs):
            k = zs * nx + (nx - 1 - x)
            for i in range(last):
                arrived(k, i)
            consume_block(k)

        each_side(s, act)

    arrived(xb, last)
    send_z(xb, last, True, True)
    ahead = 3
    fwd(1)
    fwd(2)
    fwd_last(1)
    fwd(3)
    fwd_last(2)

    for w in range(2):
        total = held[0, w]
        d_copy(0, w).wait_recv()
        total = total + drecv[0, w].astype(F32)
        for d in range(1, ny):
            y_copy(d, w).wait_recv()
            total = total + yrecv[d - 1, w].astype(F32)
        total = total.astype(BF16)
        lv[0, 2 * w * rows : 2 * (w + 1) * rows, :] = total
        lv[1, 2 * w * rows : (2 * w + 1) * rows, :] = -total[rows:]
        lv[1, (2 * w + 1) * rows : (2 * w + 2) * rows, :] = total[:rows]

    for s in range(ahead):
        consume_own(s)
    consume_other(0)
    fwd_last(ahead)
    consume_own(ahead)

    def tail(s, carry):
        fwd(s)
        fwd_last(s)
        consume_own(s)
        consume_other(s - ahead)
        return carry

    lax.fori_loop(ahead + 1, nz, tail, 0)
    for s in range(nz - ahead, nz):
        consume_other(s)

    def sent(zs, carry):
        src = zs * nx + x
        def left_z(k, i):
            @pl.when((zs <= z) & (z < nz - 1))
            def _():
                send(k, i, b + nx, up_sem.at[k, i]).wait_send()

            @pl.when((zs >= z) & (z > 0))
            def _():
                send(k, i, b - nx, dn_sem.at[k, i]).wait_send()

        for i in range(last + 1):
            left_z(src, i)
        left_z(zs * nx + (nx - 1 - x), last)
        for i in range(last):
            send(src, i, xb, x_sem.at[zs, i]).wait_send()

        @pl.when(zs == z)
        def _():
            send(src, last, xb, x_sem.at[zs, last]).wait_send()

        for v in range(nx):
            k = zs * nx + v

            @pl.when(k // per != g)
            def _():
                pltpu.make_async_remote_copy(
                    src_ref=ssend.at[k], dst_ref=srecv.at[0, 0], send_sem=s_ss.at[k],
                    recv_sem=s_rs.at[0, 0], device_id=(b, mate), device_id_type=MESH).wait_send()

        return carry

    lax.fori_loop(0, nz, sent, 0)
    for w in range(2):
        for d in range(ny):
            d_copy(d, w).wait_send()
        for d in range(1, ny):
            y_copy(d, w).wait_send()

    for p in range(per):
        for r in range(ng - 1):
            pltpu.make_async_remote_copy(
                src_ref=ssend.at[0], dst_ref=srecv.at[r, p], send_sem=s_ss.at[0],
                recv_sem=s_rs.at[r, p], device_id=(b, mate), device_id_type=MESH).wait_recv()
        for i in range(2):
            total = own[p, i]
            for r in range(ng - 1):
                total = total + srecv[r, p, i].astype(F32)
            out[i, :, p * rows : (p + 1) * rows] = total


def solution(mesh):
    nb, ng = mesh.shape["band"], mesh.shape["ga"]
    nx = 2
    nz = nb // nx
    ny = ng // 2
    per = nb // ng

    def step(elements, screened, energies, freq_points, freq_weights, band_of_slot):
        _, rows, depth = elements.shape
        quarter = screened.shape[3] // ng
        slots = energies.shape[0]
        any_space = pl.BlockSpec(memory_space=pl.ANY)
        vmem = pl.BlockSpec(memory_space=pltpu.VMEM)
        dma = pltpu.SemaphoreType.DMA
        result = pl.pallas_call(
            functools.partial(kernel, nb, ng, nx),
            out_shape=pltpu.VMEM((2, rows, per * rows), F32),
            in_specs=[any_space] * 6,
            out_specs=vmem,
            scratch_shapes=[
                pltpu.VMEM((slots,), F32), pltpu.VMEM((slots,), jnp.int32),
                pltpu.SMEM(freq_points.shape, F32), pltpu.SMEM(freq_weights.shape, F32), dma((4,)),
                pltpu.VMEM((2, nb * rows, depth), BF16),
                pltpu.VMEM((2, ng, 2, depth, quarter), BF16),
                pltpu.VMEM((2 * rows, 2 * depth), BF16),
                pltpu.VMEM((16, slots), BF16),
                pltpu.VMEM((nb, 2, rows), F32),
                pltpu.VMEM((ny, 2, 2 * rows, quarter), F32),
                pltpu.VMEM((ny, 2, 2 * rows, quarter), BF16),
                pltpu.VMEM((ny, 2, 2 * rows, quarter), BF16),
                pltpu.VMEM((ny - 1, 2, 2 * rows, quarter), BF16),
                pltpu.VMEM((ny - 1, 2, 2 * rows, quarter), BF16),
                pltpu.VMEM((2, 4 * rows, quarter), BF16),
                pltpu.VMEM((nb, 2, rows, rows), BF16),
                pltpu.VMEM((ng - 1, per, 2, rows, rows), BF16),
                pltpu.VMEM((per, 2, rows, rows), F32),
                dma, dma((2, ng)), dma((nb, 4)), dma((nb, 4)), dma((nz, 4)), dma((nb, 4)),
                dma((ny, 2)), dma((ny, 2)), dma((ny - 1, 2)), dma((ny - 1, 2)),
                dma((nb,)), dma((ng - 1, per)),
            ],
            compiler_params=pltpu.CompilerParams(
                collective_id=0, has_side_effects=True, vmem_limit_bytes=60 * 1024 * 1024),
        )(elements, screened, energies, band_of_slot, freq_points, freq_weights)
        return result

    placed = (P(None, "band", "ga"), P(None, None, "ga", None), P(), P(), P(), P())
    return jax.shard_map(
        step, mesh=mesh, in_specs=placed, out_specs=P(None, "band", "ga"), check_vma=False
    )
```

```python
import functools

import jax
import jax.numpy as jnp
from jax import lax
from jax.experimental import pallas as pl
from jax.experimental.pallas import tpu as pltpu
from jax.sharding import PartitionSpec as P

MESH = pl.DeviceIdType.MESH
F32 = jnp.float32
BF16 = jnp.bfloat16
NT = (((1,), (1,)), ((), ()))


def kernel(nb, ng, nx, el, wh, en_h, bos_h, fp_h, fw_h, out, *scratch):
    (en, bos, fp, fw, in_sem, gat, wv, a_ref, e3, scr, held, dsend, drecv, ysend, yrecv, lv, ssend, srecv, own,
     loc_sem, w_sem, up_sem, dn_sem, x_sem, g_recv, d_ss, d_rs, y_ss, y_rs, s_ss, s_rs) = scratch
    rows, depth = el.shape[1], el.shape[2]
    quarter = wh.shape[3] // ng
    nz, ny = nb // nx, ng // 2
    per = nb // ng
    slots = en.shape[0]
    b, g = lax.axis_index("band"), lax.axis_index("ga")
    z, x = b // nx, lax.rem(b, nx)
    y, c = g // 2, lax.rem(g, 2)
    mate = g + 1 - 2 * c
    xb = z * nx + (nx - 1 - x)

    barrier = pltpu.get_barrier_semaphore()

    def greet(band, ga):
        pl.semaphore_signal(barrier, inc=1, device_id=(band, ga), device_id_type=MESH)

    greet(xb, g)

    @pl.when(z > 0)
    def _():
        greet(b - nx, g)

    @pl.when(z < nz - 1)
    def _():
        greet(b + nx, g)

    for r in range(1, ng):
        greet(b, lax.rem(g + r, ng))

    small = [pltpu.make_async_copy(s, t, in_sem.at[i]) for i, (s, t) in enumerate(
        ((en_h, en), (bos_h, bos), (fp_h, fp), (fw_h, fw)))]
    mine = gat.at[:, pl.ds(pl.multiple_of(b * rows, rows), rows), :]
    local = pltpu.make_async_copy(el, mine, loc_sem)
    local.start()
    for copy in small:
        copy.start()

    def q_of(other, d):
        core = (1 - c) if other else c
        return lax.rem(y + d, ny) * 2 + core

    order = []
    for d in list(range(1, ny)) + [0]:
        order += [(1, d), (0, d)]

    def w_copy(k, w):
        o, d = order[k]
        cols = pl.ds(pl.multiple_of(q_of(o, d) * quarter, quarter), quarter)
        return pltpu.make_async_copy(wh.at[w, :, :, cols], wv.at[w, k], w_sem.at[w, k])

    below = jnp.where(z > 0, 1, 0)
    above = jnp.where(z < nz - 1, 1, 0)
    local.wait()
    for k in range(ng):
        for w in range(2):
            w_copy(k, w).start()
    pl.semaphore_wait(barrier, ng + below + above)

    unit = rows // 6
    pieces = ((0, 2 * unit), (2 * unit, 2 * unit), (4 * unit, unit), (5 * unit, unit))
    last = len(pieces) - 1

    def send(src, i, dst, sem):
        start, size = pieces[i]
        ref = gat.at[:, pl.ds(pl.multiple_of(src * rows + start, unit), size), :]
        return pltpu.make_async_remote_copy(
            src_ref=ref, dst_ref=ref, send_sem=sem, recv_sem=g_recv.at[src, i],
            device_id=(dst, g), device_id_type=MESH)

    def arrived(src, i):
        send(src, i, xb, x_sem.at[0, i]).wait_recv()

    def send_z(src, i, up, down):
        if up:
            @pl.when(z < nz - 1)
            def _():
                send(src, i, b + nx, up_sem.at[src, i]).start()

        if down:
            @pl.when(z > 0)
            def _():
                send(src, i, b - nx, dn_sem.at[src, i]).start()

    def fwd(s, only=None):
        for i in range(last) if only is None else (only,):
            for zs, up in ((z - s, True), (z + s, False)):
                @pl.when((zs >= 0) & (zs < nz))
                def _():
                    src = zs * nx + x
                    arrived(src, i)
                    send_z(src, i, up, not up)
                    send(src, i, xb, x_sem.at[zs, i]).start()

    def fwd_last(s):
        for zs, up in ((z - s, True), (z + s, False)):
            @pl.when((zs >= 0) & (zs < nz))
            def _():
                for v in (x, nx - 1 - x):
                    arrived(zs * nx + v, last)
                    send_z(zs * nx + v, last, up, not up)

    send(b, last, xb, x_sem.at[z, last]).start()
    for i in range(last + 1):
        send_z(b, i, True, True)
        if i < last:
            send(b, i, xb, x_sem.at[z, i]).start()

    for copy in small:
        copy.wait()
    row = lax.broadcasted_iota(jnp.int32, (16, slots), 0)
    e = en[...].reshape(1, slots)
    hi = e.astype(BF16).astype(F32)
    mid = (e - hi).astype(BF16).astype(F32)
    lo = e - hi - mid
    e3[...] = jnp.where(row == 0, hi, jnp.where(row == 1, mid, jnp.where(row == 2, lo, 0.0))).astype(BF16)
    tile = slots if slots <= 1024 else 8 * rows

    for u in range(slots // tile):
        slot = bos[u * tile : (u + 1) * tile].reshape(1, tile)

        def add(j, acc):
            at = pl.multiple_of(j * tile, tile)
            hit = lax.broadcasted_iota(jnp.int32, (tile, tile), 0) + at == slot
            return acc + jnp.dot(e3[:, pl.ds(at, tile)], jnp.where(hit, 1.0, 0.0).astype(BF16),
                                 preferred_element_type=F32)

        acc = lax.fori_loop(0, slots // tile, add, jnp.zeros((16, tile), F32))
        energy = jnp.sum(acc, axis=0, keepdims=True)
        for w in range(2):
            off = energy - fp[w]
            value = 0.5 * (fw[w] / (1.0 + 4.0 * off * off))
            for v in range(tile // rows):
                scr[u * (tile // rows) + v, w : w + 1, :] = value[:, v * rows : (v + 1) * rows]
    pick = lax.broadcasted_iota(jnp.int32, (rows, rows), 1) == lax.broadcasted_iota(
        jnp.int32, (rows, rows), 0)
    cols = [jnp.sum(jnp.where(pick, scr[b, w : w + 1, :], 0.0), axis=1, keepdims=True)
            for w in range(2)]

    er = gat[0, pl.ds(pl.multiple_of(b * rows, rows), rows), :]
    ei = gat[1, pl.ds(pl.multiple_of(b * rows, rows), rows), :]
    a_ref[:rows, :depth] = er
    a_ref[:rows, depth:] = ei
    a_ref[rows:, :depth] = -ei
    a_ref[rows:, depth:] = er

    def d_copy(d, w):
        return pltpu.make_async_remote_copy(
            src_ref=dsend.at[d, w], dst_ref=drecv.at[d, w], send_sem=d_ss.at[d, w],
            recv_sem=d_rs.at[d, w], device_id=(b, mate), device_id_type=MESH)

    def y_copy(d, w):
        return pltpu.make_async_remote_copy(
            src_ref=ysend.at[d - 1, w], dst_ref=yrecv.at[d - 1, w], send_sem=y_ss.at[d - 1, w],
            recv_sem=y_rs.at[d - 1, w], device_id=(b, lax.rem(y + d, ny) * 2 + c),
            device_id_type=MESH)

    def pass_on(d):
        for w in range(2):
            d_copy(d, w).wait_recv()
            ysend[d - 1, w] = (held[d, w] + drecv[d, w].astype(F32)).astype(BF16)
            y_copy(d, w).start()

    for k in range(ng):
        o, d = order[k]
        for w in range(2):
            w_copy(k, w).wait()
            part = jnp.dot(a_ref[...], wv[w, k].reshape(2 * depth, quarter),
                           preferred_element_type=F32)
            if o:
                dsend[d, w] = part.astype(BF16)
                d_copy(d, w).start()
            else:
                held[d, w] = part
        if o and k >= 2:
            pass_on(order[k - 1][1])

    def consume_block(k):
        at = pl.ds(pl.multiple_of(k * rows, rows), rows)
        pr = lax.dot_general(lv[0], gat[0, at, :], NT, preferred_element_type=F32)
        pr = pr + lax.dot_general(lv[1], gat[1, at, :], NT, preferred_element_type=F32)
        f = [cols[w] + scr[k, w : w + 1, :] for w in range(2)]
        total = [f[0] * pr[i * rows : (i + 1) * rows]
                 + f[1] * pr[(2 + i) * rows : (3 + i) * rows] for i in range(2)]
        q, p = k // per, lax.rem(k, per)

        @pl.when(q == g)
        def _():
            for i in range(2):
                own[p, i] = total[i]

        @pl.when(q != g)
        def _():
            for i in range(2):
                ssend[k, i] = total[i].astype(BF16)
            slot = lax.rem(g - q + ng, ng) - 1
            pltpu.make_async_remote_copy(
                src_ref=ssend.at[k], dst_ref=srecv.at[slot, p], send_sem=s_ss.at[k],
                recv_sem=s_rs.at[slot, p], device_id=(b, q), device_id_type=MESH).start()

    def each_side(s, act):
        @pl.when(z - s >= 0)
        def _():
            act(z - s)

        if not (isinstance(s, int) and s == 0):
            @pl.when(z + s < nz)
            def _():
                act(z + s)

    def consume_own(s):
        each_side(s, lambda zs: consume_block(zs * nx + x))

    def consume_other(s):
        def act(zs):
            k = zs * nx + (nx - 1 - x)
            for i in range(last):
                arrived(k, i)
            consume_block(k)

        each_side(s, act)

    arrived(xb, last)
    send_z(xb, last, True, True)
    ahead = 3
    fwd(1)
    fwd(2)
    fwd_last(1)
    inner = (z > 0) & (z < nz - 1)

    @pl.when(inner)
    def _():
        fwd_last(2)

    fwd(ahead, 0)

    for w in range(2):
        total = held[0, w]
        d_copy(0, w).wait_recv()
        total = total + drecv[0, w].astype(F32)
        for d in range(1, ny):
            y_copy(d, w).wait_recv()
            total = total + yrecv[d - 1, w].astype(F32)
        total = total.astype(BF16)
        lv[0, 2 * w * rows : 2 * (w + 1) * rows, :] = total
        lv[1, 2 * w * rows : (2 * w + 1) * rows, :] = -total[rows:]
        lv[1, (2 * w + 1) * rows : (2 * w + 2) * rows, :] = total[:rows]

    consume_own(0)
    consume_other(0)
    consume_own(1)
    fwd(ahead, 1)
    consume_other(1)
    fwd(ahead, 2)

    @pl.when(jnp.logical_not(inner))
    def _():
        fwd_last(2)

    consume_own(2)
    consume_other(2)
    fwd_last(ahead)
    consume_own(ahead)

    def tail(s, carry):
        fwd(s)
        fwd_last(s)
        consume_own(s)
        consume_other(s - 1)
        return carry

    lax.fori_loop(ahead + 1, nz, tail, 0)
    consume_other(nz - 1)

    def sent(zs, carry):
        src = zs * nx + x
        def left_z(k, i):
            @pl.when((zs <= z) & (z < nz - 1))
            def _():
                send(k, i, b + nx, up_sem.at[k, i]).wait_send()

            @pl.when((zs >= z) & (z > 0))
            def _():
                send(k, i, b - nx, dn_sem.at[k, i]).wait_send()

        for i in range(last + 1):
            left_z(src, i)
        left_z(zs * nx + (nx - 1 - x), last)
        for i in range(last):
            send(src, i, xb, x_sem.at[zs, i]).wait_send()

        @pl.when(zs == z)
        def _():
            send(src, last, xb, x_sem.at[zs, last]).wait_send()

        for v in range(nx):
            k = zs * nx + v

            @pl.when(k // per != g)
            def _():
                pltpu.make_async_remote_copy(
                    src_ref=ssend.at[k], dst_ref=srecv.at[0, 0], send_sem=s_ss.at[k],
                    recv_sem=s_rs.at[0, 0], device_id=(b, mate), device_id_type=MESH).wait_send()

        return carry

    lax.fori_loop(0, nz, sent, 0)
    for w in range(2):
        for d in range(ny):
            d_copy(d, w).wait_send()
        for d in range(1, ny):
            y_copy(d, w).wait_send()

    for p in range(per):
        for r in range(ng - 1):
            pltpu.make_async_remote_copy(
                src_ref=ssend.at[0], dst_ref=srecv.at[r, p], send_sem=s_ss.at[0],
                recv_sem=s_rs.at[r, p], device_id=(b, mate), device_id_type=MESH).wait_recv()
        for i in range(2):
            total = own[p, i]
            for r in range(ng - 1):
                total = total + srecv[r, p, i].astype(F32)
            out[i, :, p * rows : (p + 1) * rows] = total


def solution(mesh):
    nb, ng = mesh.shape["band"], mesh.shape["ga"]
    nx = 2
    nz = nb // nx
    ny = ng // 2
    per = nb // ng

    def step(elements, screened, energies, freq_points, freq_weights, band_of_slot):
        _, rows, depth = elements.shape
        quarter = screened.shape[3] // ng
        slots = energies.shape[0]
        any_space = pl.BlockSpec(memory_space=pl.ANY)
        vmem = pl.BlockSpec(memory_space=pltpu.VMEM)
        dma = pltpu.SemaphoreType.DMA
        result = pl.pallas_call(
            functools.partial(kernel, nb, ng, nx),
            out_shape=pltpu.VMEM((2, rows, per * rows), F32),
            in_specs=[any_space] * 6,
            out_specs=vmem,
            scratch_shapes=[
                pltpu.VMEM((slots,), F32), pltpu.VMEM((slots,), jnp.int32),
                pltpu.SMEM(freq_points.shape, F32), pltpu.SMEM(freq_weights.shape, F32), dma((4,)),
                pltpu.VMEM((2, nb * rows, depth), BF16),
                pltpu.VMEM((2, ng, 2, depth, quarter), BF16),
                pltpu.VMEM((2 * rows, 2 * depth), BF16),
                pltpu.VMEM((16, slots), BF16),
                pltpu.VMEM((nb, 2, rows), F32),
                pltpu.VMEM((ny, 2, 2 * rows, quarter), F32),
                pltpu.VMEM((ny, 2, 2 * rows, quarter), BF16),
                pltpu.VMEM((ny, 2, 2 * rows, quarter), BF16),
                pltpu.VMEM((ny - 1, 2, 2 * rows, quarter), BF16),
                pltpu.VMEM((ny - 1, 2, 2 * rows, quarter), BF16),
                pltpu.VMEM((2, 4 * rows, quarter), BF16),
                pltpu.VMEM((nb, 2, rows, rows), BF16),
                pltpu.VMEM((ng - 1, per, 2, rows, rows), BF16),
                pltpu.VMEM((per, 2, rows, rows), F32),
                dma, dma((2, ng)), dma((nb, 4)), dma((nb, 4)), dma((nz, 4)), dma((nb, 4)),
                dma((ny, 2)), dma((ny, 2)), dma((ny - 1, 2)), dma((ny - 1, 2)),
                dma((nb,)), dma((ng - 1, per)),
            ],
            compiler_params=pltpu.CompilerParams(
                collective_id=0, has_side_effects=True, vmem_limit_bytes=60 * 1024 * 1024),
        )(elements, screened, energies, band_of_slot, freq_points, freq_weights)
        return result

    placed = (P(None, "band", "ga"), P(None, None, "ga", None), P(), P(), P(), P())
    return jax.shard_map(
        step, mesh=mesh, in_specs=placed, out_specs=P(None, "band", "ga"), check_vma=False
    )
```

```python
import functools

import jax
import jax.numpy as jnp
from jax import lax
from jax.experimental import pallas as pl
from jax.experimental.pallas import tpu as pltpu
from jax.sharding import PartitionSpec as P

MESH = pl.DeviceIdType.MESH
F32 = jnp.float32
BF16 = jnp.bfloat16
NT = (((1,), (1,)), ((), ()))


def kernel(nb, ng, nx, el, wh, en_h, bos_h, fp_h, fw_h, out, *scratch):
    (en, bos, fp, fw, in_sem, gat, wv, a_ref, e3, scr, held, dsend, drecv, ysend, yrecv, lv, ssend, srecv, own,
     loc_sem, w_sem, up_sem, dn_sem, x_sem, g_recv, d_ss, d_rs, y_ss, y_rs, s_ss, s_rs) = scratch
    rows, depth = el.shape[1], el.shape[2]
    quarter = wh.shape[3] // ng
    nz, ny = nb // nx, ng // 2
    per = nb // ng
    slots = en.shape[0]
    b, g = lax.axis_index("band"), lax.axis_index("ga")
    z, x = b // nx, lax.rem(b, nx)
    y, c = g // 2, lax.rem(g, 2)
    mate = g + 1 - 2 * c
    xb = z * nx + (nx - 1 - x)

    barrier = pltpu.get_barrier_semaphore()

    def greet(band, ga):
        pl.semaphore_signal(barrier, inc=1, device_id=(band, ga), device_id_type=MESH)

    greet(xb, g)

    @pl.when(z > 0)
    def _():
        greet(b - nx, g)

    @pl.when(z < nz - 1)
    def _():
        greet(b + nx, g)

    for r in range(1, ng):
        greet(b, lax.rem(g + r, ng))

    small = [pltpu.make_async_copy(s, t, in_sem.at[i]) for i, (s, t) in enumerate(
        ((en_h, en), (bos_h, bos), (fp_h, fp), (fw_h, fw)))]
    mine = gat.at[:, pl.ds(pl.multiple_of(b * rows, rows), rows), :]
    local = pltpu.make_async_copy(el, mine, loc_sem)
    local.start()
    for copy in small:
        copy.start()

    def q_of(other, d):
        core = (1 - c) if other else c
        return lax.rem(y + d, ny) * 2 + core

    order = []
    for d in list(range(1, ny)) + [0]:
        order += [(1, d), (0, d)]

    def w_copy(k, w):
        o, d = order[k]
        cols = pl.ds(pl.multiple_of(q_of(o, d) * quarter, quarter), quarter)
        return pltpu.make_async_copy(wh.at[w, :, :, cols], wv.at[w, k], w_sem.at[w, k])

    below = jnp.where(z > 0, 1, 0)
    above = jnp.where(z < nz - 1, 1, 0)
    local.wait()
    for k in range(ng):
        for w in range(2):
            w_copy(k, w).start()
    pl.semaphore_wait(barrier, ng + below + above)

    unit = rows // 6
    pieces = ((0, 2 * unit), (2 * unit, 2 * unit), (4 * unit, unit), (5 * unit, unit))
    last = len(pieces) - 1

    def send(src, i, dst, sem):
        start, size = pieces[i]
        ref = gat.at[:, pl.ds(pl.multiple_of(src * rows + start, unit), size), :]
        return pltpu.make_async_remote_copy(
            src_ref=ref, dst_ref=ref, send_sem=sem, recv_sem=g_recv.at[src, i],
            device_id=(dst, g), device_id_type=MESH)

    def arrived(src, i):
        send(src, i, xb, x_sem.at[0, i]).wait_recv()

    def send_z(src, i, up, down):
        if up:
            @pl.when(z < nz - 1)
            def _():
                send(src, i, b + nx, up_sem.at[src, i]).start()

        if down:
            @pl.when(z > 0)
            def _():
                send(src, i, b - nx, dn_sem.at[src, i]).start()

    def fwd(s, only=None):
        for i in range(last) if only is None else (only,):
            for zs, up in ((z - s, True), (z + s, False)):
                @pl.when((zs >= 0) & (zs < nz))
                def _():
                    src = zs * nx + x
                    arrived(src, i)
                    send_z(src, i, up, not up)
                    send(src, i, xb, x_sem.at[zs, i]).start()

    def fwd_last(s):
        for zs, up in ((z - s, True), (z + s, False)):
            @pl.when((zs >= 0) & (zs < nz))
            def _():
                for v in (x, nx - 1 - x):
                    arrived(zs * nx + v, last)
                    send_z(zs * nx + v, last, up, not up)

    send(b, last, xb, x_sem.at[z, last]).start()
    for i in range(last):
        send_z(b, i, True, True)
        send(b, i, xb, x_sem.at[z, i]).start()

    for copy in small:
        copy.wait()
    row = lax.broadcasted_iota(jnp.int32, (16, slots), 0)
    e = en[...].reshape(1, slots)
    hi = e.astype(BF16).astype(F32)
    mid = (e - hi).astype(BF16).astype(F32)
    lo = e - hi - mid
    e3[...] = jnp.where(row == 0, hi, jnp.where(row == 1, mid, jnp.where(row == 2, lo, 0.0))).astype(BF16)
    tile = slots if slots <= 1024 else 8 * rows

    for u in range(slots // tile):
        slot = bos[u * tile : (u + 1) * tile].reshape(1, tile)

        def add(j, acc):
            at = pl.multiple_of(j * tile, tile)
            hit = lax.broadcasted_iota(jnp.int32, (tile, tile), 0) + at == slot
            return acc + jnp.dot(e3[:, pl.ds(at, tile)], jnp.where(hit, 1.0, 0.0).astype(BF16),
                                 preferred_element_type=F32)

        acc = lax.fori_loop(0, slots // tile, add, jnp.zeros((16, tile), F32))
        energy = jnp.sum(acc, axis=0, keepdims=True)
        for w in range(2):
            off = energy - fp[w]
            value = 0.5 * (fw[w] / (1.0 + 4.0 * off * off))
            for v in range(tile // rows):
                scr[u * (tile // rows) + v, w : w + 1, :] = value[:, v * rows : (v + 1) * rows]
    pick = lax.broadcasted_iota(jnp.int32, (rows, rows), 1) == lax.broadcasted_iota(
        jnp.int32, (rows, rows), 0)
    cols = [jnp.sum(jnp.where(pick, scr[b, w : w + 1, :], 0.0), axis=1, keepdims=True)
            for w in range(2)]

    er = gat[0, pl.ds(pl.multiple_of(b * rows, rows), rows), :]
    ei = gat[1, pl.ds(pl.multiple_of(b * rows, rows), rows), :]
    a_ref[:rows, :depth] = er
    a_ref[:rows, depth:] = ei
    a_ref[rows:, :depth] = -ei
    a_ref[rows:, depth:] = er

    def d_copy(d, w):
        return pltpu.make_async_remote_copy(
            src_ref=dsend.at[d, w], dst_ref=drecv.at[d, w], send_sem=d_ss.at[d, w],
            recv_sem=d_rs.at[d, w], device_id=(b, mate), device_id_type=MESH)

    def y_copy(d, w):
        return pltpu.make_async_remote_copy(
            src_ref=ysend.at[d - 1, w], dst_ref=yrecv.at[d - 1, w], send_sem=y_ss.at[d - 1, w],
            recv_sem=y_rs.at[d - 1, w], device_id=(b, lax.rem(y + d, ny) * 2 + c),
            device_id_type=MESH)

    def pass_on(d):
        for w in range(2):
            d_copy(d, w).wait_recv()
            ysend[d - 1, w] = (held[d, w] + drecv[d, w].astype(F32)).astype(BF16)
            y_copy(d, w).start()

    for k in range(ng):
        o, d = order[k]
        for w in range(2):
            w_copy(k, w).wait()
            part = jnp.dot(a_ref[...], wv[w, k].reshape(2 * depth, quarter),
                           preferred_element_type=F32)
            if o:
                dsend[d, w] = part.astype(BF16)
                d_copy(d, w).start()
            else:
                held[d, w] = part
        if d and not o:
            pass_on(d)

    def consume_block(k):
        at = pl.ds(pl.multiple_of(k * rows, rows), rows)
        pr = lax.dot_general(lv[0], gat[0, at, :], NT, preferred_element_type=F32)
        pr = pr + lax.dot_general(lv[1], gat[1, at, :], NT, preferred_element_type=F32)
        f = [cols[w] + scr[k, w : w + 1, :] for w in range(2)]
        total = [f[0] * pr[i * rows : (i + 1) * rows]
                 + f[1] * pr[(2 + i) * rows : (3 + i) * rows] for i in range(2)]
        q, p = k // per, lax.rem(k, per)

        @pl.when(q == g)
        def _():
            for i in range(2):
                own[p, i] = total[i]

        @pl.when(q != g)
        def _():
            for i in range(2):
                ssend[k, i] = total[i].astype(BF16)
            slot = lax.rem(g - q + ng, ng) - 1
            pltpu.make_async_remote_copy(
                src_ref=ssend.at[k], dst_ref=srecv.at[slot, p], send_sem=s_ss.at[k],
                recv_sem=s_rs.at[slot, p], device_id=(b, q), device_id_type=MESH).start()

    def each_side(s, act):
        @pl.when(z - s >= 0)
        def _():
            act(z - s)

        if not (isinstance(s, int) and s == 0):
            @pl.when(z + s < nz)
            def _():
                act(z + s)

    def consume_own(s):
        each_side(s, lambda zs: consume_block(zs * nx + x))

    def consume_other(s):
        def act(zs):
            k = zs * nx + (nx - 1 - x)
            for i in range(last):
                arrived(k, i)
            consume_block(k)

        each_side(s, act)

    ahead = 3
    fwd(1)
    fwd(2)
    send_z(b, last, True, True)
    arrived(xb, last)
    send_z(xb, last, True, True)
    fwd_last(1)
    inner = (z > 0) & (z < nz - 1)

    @pl.when(inner)
    def _():
        fwd_last(2)

    fwd(ahead, 0)
    fwd(ahead, 1)

    for w in range(2):
        total = held[0, w]
        d_copy(0, w).wait_recv()
        total = total + drecv[0, w].astype(F32)
        for d in range(1, ny):
            y_copy(d, w).wait_recv()
            total = total + yrecv[d - 1, w].astype(F32)
        total = total.astype(BF16)
        lv[0, 2 * w * rows : 2 * (w + 1) * rows, :] = total
        lv[1, 2 * w * rows : (2 * w + 1) * rows, :] = -total[rows:]
        lv[1, (2 * w + 1) * rows : (2 * w + 2) * rows, :] = total[:rows]

    consume_own(0)
    consume_other(0)
    fwd(ahead, 2)
    consume_own(1)
    consume_other(1)

    @pl.when(jnp.logical_not(inner))
    def _():
        fwd_last(2)

    consume_own(2)
    consume_other(2)
    fwd_last(ahead)
    consume_own(ahead)

    def tail(s, carry):
        fwd(s)
        fwd_last(s)
        consume_own(s)
        consume_other(s - 1)
        return carry

    lax.fori_loop(ahead + 1, nz, tail, 0)
    consume_other(nz - 1)

    def sent(zs, carry):
        src = zs * nx + x
        def left_z(k, i):
            @pl.when((zs <= z) & (z < nz - 1))
            def _():
                send(k, i, b + nx, up_sem.at[k, i]).wait_send()

            @pl.when((zs >= z) & (z > 0))
            def _():
                send(k, i, b - nx, dn_sem.at[k, i]).wait_send()

        for i in range(last + 1):
            left_z(src, i)
        left_z(zs * nx + (nx - 1 - x), last)
        for i in range(last):
            send(src, i, xb, x_sem.at[zs, i]).wait_send()

        @pl.when(zs == z)
        def _():
            send(src, last, xb, x_sem.at[zs, last]).wait_send()

        for v in range(nx):
            k = zs * nx + v

            @pl.when(k // per != g)
            def _():
                pltpu.make_async_remote_copy(
                    src_ref=ssend.at[k], dst_ref=srecv.at[0, 0], send_sem=s_ss.at[k],
                    recv_sem=s_rs.at[0, 0], device_id=(b, mate), device_id_type=MESH).wait_send()

        return carry

    lax.fori_loop(0, nz, sent, 0)
    for w in range(2):
        for d in range(ny):
            d_copy(d, w).wait_send()
        for d in range(1, ny):
            y_copy(d, w).wait_send()

    for p in range(per):
        for r in range(ng - 1):
            pltpu.make_async_remote_copy(
                src_ref=ssend.at[0], dst_ref=srecv.at[r, p], send_sem=s_ss.at[0],
                recv_sem=s_rs.at[r, p], device_id=(b, mate), device_id_type=MESH).wait_recv()
        for i in range(2):
            total = own[p, i]
            for r in range(ng - 1):
                total = total + srecv[r, p, i].astype(F32)
            out[i, :, p * rows : (p + 1) * rows] = total


def solution(mesh):
    nb, ng = mesh.shape["band"], mesh.shape["ga"]
    nx = 2
    nz = nb // nx
    ny = ng // 2
    per = nb // ng

    def step(elements, screened, energies, freq_points, freq_weights, band_of_slot):
        _, rows, depth = elements.shape
        quarter = screened.shape[3] // ng
        slots = energies.shape[0]
        any_space = pl.BlockSpec(memory_space=pl.ANY)
        vmem = pl.BlockSpec(memory_space=pltpu.VMEM)
        dma = pltpu.SemaphoreType.DMA
        result = pl.pallas_call(
            functools.partial(kernel, nb, ng, nx),
            out_shape=pltpu.VMEM((2, rows, per * rows), F32),
            in_specs=[any_space] * 6,
            out_specs=vmem,
            scratch_shapes=[
                pltpu.VMEM((slots,), F32), pltpu.VMEM((slots,), jnp.int32),
                pltpu.SMEM(freq_points.shape, F32), pltpu.SMEM(freq_weights.shape, F32), dma((4,)),
                pltpu.VMEM((2, nb * rows, depth), BF16),
                pltpu.VMEM((2, ng, 2, depth, quarter), BF16),
                pltpu.VMEM((2 * rows, 2 * depth), BF16),
                pltpu.VMEM((16, slots), BF16),
                pltpu.VMEM((nb, 2, rows), F32),
                pltpu.VMEM((ny, 2, 2 * rows, quarter), F32),
                pltpu.VMEM((ny, 2, 2 * rows, quarter), BF16),
                pltpu.VMEM((ny, 2, 2 * rows, quarter), BF16),
                pltpu.VMEM((ny - 1, 2, 2 * rows, quarter), BF16),
                pltpu.VMEM((ny - 1, 2, 2 * rows, quarter), BF16),
                pltpu.VMEM((2, 4 * rows, quarter), BF16),
                pltpu.VMEM((nb, 2, rows, rows), BF16),
                pltpu.VMEM((ng - 1, per, 2, rows, rows), BF16),
                pltpu.VMEM((per, 2, rows, rows), F32),
                dma, dma((2, ng)), dma((nb, 4)), dma((nb, 4)), dma((nz, 4)), dma((nb, 4)),
                dma((ny, 2)), dma((ny, 2)), dma((ny - 1, 2)), dma((ny - 1, 2)),
                dma((nb,)), dma((ng - 1, per)),
            ],
            compiler_params=pltpu.CompilerParams(
                collective_id=0, has_side_effects=True, vmem_limit_bytes=60 * 1024 * 1024),
        )(elements, screened, energies, band_of_slot, freq_points, freq_weights)
        return result

    placed = (P(None, "band", "ga"), P(None, None, "ga", None), P(), P(), P(), P())
    return jax.shard_map(
        step, mesh=mesh, in_specs=placed, out_specs=P(None, "band", "ga"), check_vma=False
    )
```

```python
import functools

import jax
import jax.numpy as jnp
from jax import lax
from jax.experimental import pallas as pl
from jax.experimental.pallas import tpu as pltpu
from jax.sharding import PartitionSpec as P

MESH = pl.DeviceIdType.MESH
F32 = jnp.float32
BF16 = jnp.bfloat16
NT = (((1,), (1,)), ((), ()))


def kernel(nb, ng, nx, el, wh, en_h, bos_h, fp_h, fw_h, out, *scratch):
    (en, bos, fp, fw, in_sem, gat, wv, a_ref, e3, scr, held, dsend, drecv, ysend, yrecv, lv, ssend, srecv, own,
     loc_sem, w_sem, up_sem, dn_sem, x_sem, g_recv, d_ss, d_rs, y_ss, y_rs, s_ss, s_rs) = scratch
    rows, depth = el.shape[1], el.shape[2]
    quarter = wh.shape[3] // ng
    nz, ny = nb // nx, ng // 2
    per = nb // ng
    slots = en.shape[0]
    b, g = lax.axis_index("band"), lax.axis_index("ga")
    z, x = b // nx, lax.rem(b, nx)
    y, c = g // 2, lax.rem(g, 2)
    mate = g + 1 - 2 * c
    xb = z * nx + (nx - 1 - x)

    barrier = pltpu.get_barrier_semaphore()

    def greet(band, ga):
        pl.semaphore_signal(barrier, inc=1, device_id=(band, ga), device_id_type=MESH)

    greet(xb, g)

    @pl.when(z > 0)
    def _():
        greet(b - nx, g)

    @pl.when(z < nz - 1)
    def _():
        greet(b + nx, g)

    for r in range(1, ng):
        greet(b, lax.rem(g + r, ng))

    small = [pltpu.make_async_copy(s, t, in_sem.at[i]) for i, (s, t) in enumerate(
        ((en_h, en), (bos_h, bos), (fp_h, fp), (fw_h, fw)))]
    mine = gat.at[:, pl.ds(pl.multiple_of(b * rows, rows), rows), :]
    local = pltpu.make_async_copy(el, mine, loc_sem)
    local.start()
    for copy in small:
        copy.start()

    def q_of(other, d):
        core = (1 - c) if other else c
        return lax.rem(y + d, ny) * 2 + core

    order = []
    for d in list(range(1, ny)) + [0]:
        order += [(1, d), (0, d)]

    def w_copy(k, w):
        o, d = order[k]
        cols = pl.ds(pl.multiple_of(q_of(o, d) * quarter, quarter), quarter)
        return pltpu.make_async_copy(wh.at[w, :, :, cols], wv.at[w, k], w_sem.at[w, k])

    below = jnp.where(z > 0, 1, 0)
    above = jnp.where(z < nz - 1, 1, 0)
    local.wait()
    for k in range(ng):
        for w in range(2):
            w_copy(k, w).start()
    pl.semaphore_wait(barrier, ng + below + above)

    unit = rows // 6
    pieces = ((0, 2 * unit), (2 * unit, 2 * unit), (4 * unit, unit), (5 * unit, unit))
    last = len(pieces) - 1

    def send(src, i, dst, sem):
        start, size = pieces[i]
        ref = gat.at[:, pl.ds(pl.multiple_of(src * rows + start, unit), size), :]
        return pltpu.make_async_remote_copy(
            src_ref=ref, dst_ref=ref, send_sem=sem, recv_sem=g_recv.at[src, i],
            device_id=(dst, g), device_id_type=MESH)

    def arrived(src, i):
        send(src, i, xb, x_sem.at[0, i]).wait_recv()

    def send_z(src, i, up, down):
        if up:
            @pl.when(z < nz - 1)
            def _():
                send(src, i, b + nx, up_sem.at[src, i]).start()

        if down:
            @pl.when(z > 0)
            def _():
                send(src, i, b - nx, dn_sem.at[src, i]).start()

    def fwd(s, only=None):
        for i in range(last) if only is None else (only,):
            for zs, up in ((z - s, True), (z + s, False)):
                @pl.when((zs >= 0) & (zs < nz))
                def _():
                    src = zs * nx + x
                    arrived(src, i)
                    send_z(src, i, up, not up)
                    send(src, i, xb, x_sem.at[zs, i]).start()

    def fwd_last(s):
        for zs, up in ((z - s, True), (z + s, False)):
            @pl.when((zs >= 0) & (zs < nz))
            def _():
                for v in (x, nx - 1 - x):
                    arrived(zs * nx + v, last)
                    send_z(zs * nx + v, last, up, not up)

    send(b, last, xb, x_sem.at[z, last]).start()
    for i in range(last):
        send_z(b, i, True, True)
        send(b, i, xb, x_sem.at[z, i]).start()
    inner = (z > 0) & (z < nz - 1)
    outer = jnp.logical_not(inner)

    @pl.when(outer)
    def _():
        send_z(b, last, True, True)

    for copy in small:
        copy.wait()
    row = lax.broadcasted_iota(jnp.int32, (16, slots), 0)
    e = en[...].reshape(1, slots)
    hi = e.astype(BF16).astype(F32)
    mid = (e - hi).astype(BF16).astype(F32)
    lo = e - hi - mid
    e3[...] = jnp.where(row == 0, hi, jnp.where(row == 1, mid, jnp.where(row == 2, lo, 0.0))).astype(BF16)
    tile = slots if slots <= 1024 else 8 * rows

    for u in range(slots // tile):
        slot = bos[u * tile : (u + 1) * tile].reshape(1, tile)

        def add(j, acc):
            at = pl.multiple_of(j * tile, tile)
            hit = lax.broadcasted_iota(jnp.int32, (tile, tile), 0) + at == slot
            return acc + jnp.dot(e3[:, pl.ds(at, tile)], jnp.where(hit, 1.0, 0.0).astype(BF16),
                                 preferred_element_type=F32)

        acc = lax.fori_loop(0, slots // tile, add, jnp.zeros((16, tile), F32))
        energy = jnp.sum(acc, axis=0, keepdims=True)
        for w in range(2):
            off = energy - fp[w]
            value = 0.5 * (fw[w] / (1.0 + 4.0 * off * off))
            for v in range(tile // rows):
                scr[u * (tile // rows) + v, w : w + 1, :] = value[:, v * rows : (v + 1) * rows]
    pick = lax.broadcasted_iota(jnp.int32, (rows, rows), 1) == lax.broadcasted_iota(
        jnp.int32, (rows, rows), 0)
    cols = [jnp.sum(jnp.where(pick, scr[b, w : w + 1, :], 0.0), axis=1, keepdims=True)
            for w in range(2)]

    er = gat[0, pl.ds(pl.multiple_of(b * rows, rows), rows), :]
    ei = gat[1, pl.ds(pl.multiple_of(b * rows, rows), rows), :]
    a_ref[:rows, :depth] = er
    a_ref[:rows, depth:] = ei
    a_ref[rows:, :depth] = -ei
    a_ref[rows:, depth:] = er

    def d_copy(d, w):
        return pltpu.make_async_remote_copy(
            src_ref=dsend.at[d, w], dst_ref=drecv.at[d, w], send_sem=d_ss.at[d, w],
            recv_sem=d_rs.at[d, w], device_id=(b, mate), device_id_type=MESH)

    def y_copy(d, w):
        return pltpu.make_async_remote_copy(
            src_ref=ysend.at[d - 1, w], dst_ref=yrecv.at[d - 1, w], send_sem=y_ss.at[d - 1, w],
            recv_sem=y_rs.at[d - 1, w], device_id=(b, lax.rem(y + d, ny) * 2 + c),
            device_id_type=MESH)

    def pass_on(d):
        for w in range(2):
            d_copy(d, w).wait_recv()
            ysend[d - 1, w] = (held[d, w] + drecv[d, w].astype(F32)).astype(BF16)
            y_copy(d, w).start()

    for k in range(ng):
        o, d = order[k]
        for w in range(2):
            w_copy(k, w).wait()
            part = jnp.dot(a_ref[...], wv[w, k].reshape(2 * depth, quarter),
                           preferred_element_type=F32)
            if o:
                dsend[d, w] = part.astype(BF16)
                d_copy(d, w).start()
            else:
                held[d, w] = part
        if d and not o:
            pass_on(d)

    def consume_block(k):
        at = pl.ds(pl.multiple_of(k * rows, rows), rows)
        pr = lax.dot_general(lv[0], gat[0, at, :], NT, preferred_element_type=F32)
        pr = pr + lax.dot_general(lv[1], gat[1, at, :], NT, preferred_element_type=F32)
        f = [cols[w] + scr[k, w : w + 1, :] for w in range(2)]
        total = [f[0] * pr[i * rows : (i + 1) * rows]
                 + f[1] * pr[(2 + i) * rows : (3 + i) * rows] for i in range(2)]
        q, p = k // per, lax.rem(k, per)

        @pl.when(q == g)
        def _():
            for i in range(2):
                own[p, i] = total[i]

        @pl.when(q != g)
        def _():
            for i in range(2):
                ssend[k, i] = total[i].astype(BF16)
            slot = lax.rem(g - q + ng, ng) - 1
            pltpu.make_async_remote_copy(
                src_ref=ssend.at[k], dst_ref=srecv.at[slot, p], send_sem=s_ss.at[k],
                recv_sem=s_rs.at[slot, p], device_id=(b, q), device_id_type=MESH).start()

    def each_side(s, act):
        @pl.when(z - s >= 0)
        def _():
            act(z - s)

        if not (isinstance(s, int) and s == 0):
            @pl.when(z + s < nz)
            def _():
                act(z + s)

    def consume_own(s):
        each_side(s, lambda zs: consume_block(zs * nx + x))

    def consume_other(s):
        def act(zs):
            k = zs * nx + (nx - 1 - x)
            for i in range(last):
                arrived(k, i)
            consume_block(k)

        each_side(s, act)

    ahead = 3

    def mine_last():
        arrived(xb, last)
        send_z(xb, last, True, True)

    pl.when(outer)(mine_last)
    fwd(1)
    fwd(2)

    @pl.when(inner)
    def _():
        send_z(b, last, True, True)
        mine_last()
        fwd_last(1)
        fwd_last(2)

    fwd(ahead, 0)
    fwd(ahead, 1)

    for w in range(2):
        total = held[0, w]
        d_copy(0, w).wait_recv()
        total = total + drecv[0, w].astype(F32)
        for d in range(1, ny):
            y_copy(d, w).wait_recv()
            total = total + yrecv[d - 1, w].astype(F32)
        total = total.astype(BF16)
        lv[0, 2 * w * rows : 2 * (w + 1) * rows, :] = total
        lv[1, 2 * w * rows : (2 * w + 1) * rows, :] = -total[rows:]
        lv[1, (2 * w + 1) * rows : (2 * w + 2) * rows, :] = total[:rows]

    consume_own(0)
    consume_other(0)
    fwd(ahead, 2)
    pl.when(outer)(lambda: fwd_last(1))
    consume_own(1)
    consume_other(1)
    pl.when(outer)(lambda: fwd_last(2))
    consume_own(2)
    consume_other(2)
    fwd_last(ahead)
    consume_own(ahead)

    def tail(s, carry):
        fwd(s)
        fwd_last(s)
        consume_own(s)
        consume_other(s - 1)
        return carry

    lax.fori_loop(ahead + 1, nz, tail, 0)
    consume_other(nz - 1)

    def sent(zs, carry):
        src = zs * nx + x
        def left_z(k, i):
            @pl.when((zs <= z) & (z < nz - 1))
            def _():
                send(k, i, b + nx, up_sem.at[k, i]).wait_send()

            @pl.when((zs >= z) & (z > 0))
            def _():
                send(k, i, b - nx, dn_sem.at[k, i]).wait_send()

        for i in range(last + 1):
            left_z(src, i)
        left_z(zs * nx + (nx - 1 - x), last)
        for i in range(last):
            send(src, i, xb, x_sem.at[zs, i]).wait_send()

        @pl.when(zs == z)
        def _():
            send(src, last, xb, x_sem.at[zs, last]).wait_send()

        for v in range(nx):
            k = zs * nx + v

            @pl.when(k // per != g)
            def _():
                pltpu.make_async_remote_copy(
                    src_ref=ssend.at[k], dst_ref=srecv.at[0, 0], send_sem=s_ss.at[k],
                    recv_sem=s_rs.at[0, 0], device_id=(b, mate), device_id_type=MESH).wait_send()

        return carry

    lax.fori_loop(0, nz, sent, 0)
    for w in range(2):
        for d in range(ny):
            d_copy(d, w).wait_send()
        for d in range(1, ny):
            y_copy(d, w).wait_send()

    for p in range(per):
        for r in range(ng - 1):
            pltpu.make_async_remote_copy(
                src_ref=ssend.at[0], dst_ref=srecv.at[r, p], send_sem=s_ss.at[0],
                recv_sem=s_rs.at[r, p], device_id=(b, mate), device_id_type=MESH).wait_recv()
        for i in range(2):
            total = own[p, i]
            for r in range(ng - 1):
                total = total + srecv[r, p, i].astype(F32)
            out[i, :, p * rows : (p + 1) * rows] = total


def solution(mesh):
    nb, ng = mesh.shape["band"], mesh.shape["ga"]
    nx = 2
    nz = nb // nx
    ny = ng // 2
    per = nb // ng

    def step(elements, screened, energies, freq_points, freq_weights, band_of_slot):
        _, rows, depth = elements.shape
        quarter = screened.shape[3] // ng
        slots = energies.shape[0]
        any_space = pl.BlockSpec(memory_space=pl.ANY)
        vmem = pl.BlockSpec(memory_space=pltpu.VMEM)
        dma = pltpu.SemaphoreType.DMA
        result = pl.pallas_call(
            functools.partial(kernel, nb, ng, nx),
            out_shape=pltpu.VMEM((2, rows, per * rows), F32),
            in_specs=[any_space] * 6,
            out_specs=vmem,
            scratch_shapes=[
                pltpu.VMEM((slots,), F32), pltpu.VMEM((slots,), jnp.int32),
                pltpu.SMEM(freq_points.shape, F32), pltpu.SMEM(freq_weights.shape, F32), dma((4,)),
                pltpu.VMEM((2, nb * rows, depth), BF16),
                pltpu.VMEM((2, ng, 2, depth, quarter), BF16),
                pltpu.VMEM((2 * rows, 2 * depth), BF16),
                pltpu.VMEM((16, slots), BF16),
                pltpu.VMEM((nb, 2, rows), F32),
                pltpu.VMEM((ny, 2, 2 * rows, quarter), F32),
                pltpu.VMEM((ny, 2, 2 * rows, quarter), BF16),
                pltpu.VMEM((ny, 2, 2 * rows, quarter), BF16),
                pltpu.VMEM((ny - 1, 2, 2 * rows, quarter), BF16),
                pltpu.VMEM((ny - 1, 2, 2 * rows, quarter), BF16),
                pltpu.VMEM((2, 4 * rows, quarter), BF16),
                pltpu.VMEM((nb, 2, rows, rows), BF16),
                pltpu.VMEM((ng - 1, per, 2, rows, rows), BF16),
                pltpu.VMEM((per, 2, rows, rows), F32),
                dma, dma((2, ng)), dma((nb, 4)), dma((nb, 4)), dma((nz, 4)), dma((nb, 4)),
                dma((ny, 2)), dma((ny, 2)), dma((ny - 1, 2)), dma((ny - 1, 2)),
                dma((nb,)), dma((ng - 1, per)),
            ],
            compiler_params=pltpu.CompilerParams(
                collective_id=0, has_side_effects=True, vmem_limit_bytes=60 * 1024 * 1024),
        )(elements, screened, energies, band_of_slot, freq_points, freq_weights)
        return result

    placed = (P(None, "band", "ga"), P(None, None, "ga", None), P(), P(), P(), P())
    return jax.shard_map(
        step, mesh=mesh, in_specs=placed, out_specs=P(None, "band", "ga"), check_vma=False
    )
```
